256 devices in a mesh: grp: 2 (over y), theta: 64 (over z, x), phi: 2 (over core).
Axes of the slice: x: 4, y: 2, z: 16, core: 2. Of those that a mesh axis runs over, the one named last changes fastest.
The devices are a block of a 4x16x16 slice.
Arguments:
- maps: bfloat16 [8, 4096, 4096], P('grp', 'theta', 'phi'), parts along dimension 0, may hold values from -6 to 6
- deltas: bfloat16 [4096, 4, 4096], P('phi', None, 'theta'), may hold values from -1 to 1
- spin_rows: bfloat16 [4096, 2, 4], P('phi'), may hold values from -1 to 1
- ell_index: int32 [4], replicated, may hold values from 1024 to 2047
- owner_map: int32 [4096], replicated, may hold values from 0 to 4095, each once
- prior: float32 [4], replicated, may hold values from 0.3 to 3
Outputs:
- gradient: float32 [8, 2, 4096], P('grp', None, ('theta', 'phi')), parts along dimension 0
The draws below stay inside these ranges and needn't reach their ends.
There are 2 independent parts, one for each index of `grp`. The reference program is written for one: setup_inputs(seed, part) draws one part's arguments, and reference() takes and returns one part's arrays. A program takes and returns all parts, laid end to end along the dimension named above; an argument that names none is the same for every part. Nothing has to cross between parts.
Inputs may be any that keep to these rules, and one draw needn't show every extreme that they name: `ell_index`: every selected degree is at least 1024; tables may repeat a degree. A permutation of the Fourier indices; slot s of deltas and of the output belongs to the frequency owner_map[s].
All inputs are finite; a program needn't handle non-finite values.
Results may differ from the reference program's by a relative error of at most 0.0003.
Values may be sent and summed in bfloat16 or wider, within the bound.
A program may use at most 128 MiB of HBM per device.

```python
import math
import jax
import jax.numpy as jnp
from jax import lax

L = 2048
NL = 4


def touch_ends(result, rng, low, top_value):
    place = [jax.random.randint(jax.random.fold_in(rng, axis), (), 0, length) for axis, length in enumerate(result.shape)]
    longest = result.shape.index(max(result.shape))
    beside = place[:longest] + [(place[longest] + 1) % result.shape[longest]] + place[longest + 1:]
    return result.at[tuple(place)].set(low).at[tuple(beside)].set(top_value)


def shard_levels(rng, dims, shards, low, high):
    factor_of, own = 1.0, jax.random.fold_in(rng, 6)
    for dim, parts in shards:
        steps = jnp.exp(jax.random.uniform(jax.random.fold_in(own, dim), (parts,), jnp.float32, low / len(shards), high / len(shards)))
        factor_of = factor_of * jnp.repeat(steps, dims[dim] // parts).reshape([-1 if axis == dim else 1 for axis in range(len(dims))])
    return factor_of


def bell_draw(rng, dims, width, limit, pieces=(), kind=jnp.bfloat16):
    array = width * jax.random.normal(rng, dims, jnp.float32)
    if pieces:
        array = array * shard_levels(rng, dims, pieces, -0.22, 0.18)
    return jnp.clip(array, -limit, limit).astype(kind)


def setup_inputs(seed: int = 0, part: int = 0) -> dict:
    streams_of = jax.random.split(jax.random.key(seed), 7)
    part_keys = jax.random.split(jax.random.fold_in(streams_of[6], part), 7)
    maps = bell_draw(part_keys[0], (4, 2 * L, 2 * L), 1.0, 6.0, ((1, 64), (2, 2)))
    deltas = jnp.clip(jax.random.uniform(streams_of[1], (2 * L, NL, 2 * L), jnp.float32, -1.0, 1.0) * shard_levels(streams_of[1], (2 * L, NL, 2 * L), ((0, 2), (2, 64)), -0.4, 0.0), -1.0, 1.0).astype(jnp.bfloat16)
    spin_rows = jnp.clip(jax.random.uniform(streams_of[2], (2 * L, 2, NL), jnp.float32, -1.0, 1.0) * shard_levels(streams_of[2], (2 * L, 2, NL), ((0, 2),), -0.4, 0.0), -1.0, 1.0).astype(jnp.bfloat16)
    ell_index = touch_ends(jax.random.randint(streams_of[3], (NL,), L // 2, L), jax.random.fold_in(streams_of[3], 1), L // 2, L - 1).astype(jnp.int32)
    owner_map = jax.random.permutation(streams_of[4], 2 * L).astype(jnp.int32)
    prior = jnp.clip(jnp.exp(jax.random.uniform(streams_of[5], (NL,), jnp.float32, math.log(0.3), math.log(3.0))), 0.3, 3.0)
    return dict(maps=maps, deltas=deltas, spin_rows=spin_rows, ell_index=ell_index, owner_map=owner_map, prior=prior)


def signed_freq(length):
    positions = jnp.arange(length, dtype=jnp.int32)
    return jnp.where(positions < length // 2, positions, positions - length)

def reference(maps, deltas, spin_rows, ell_index, owner_map, prior):
    length = 2 * L
    values = maps.astype(jnp.float32)
    prod_real = values[1] * values[2]
    prod_imag = values[1] * values[3]
    scalar_spec = jnp.fft.fft2(values[0]) / length
    spin_spec = jnp.fft.fft2(lax.complex(prod_real, prod_imag)) / length
    planes = [jnp.real(scalar_spec)[:, owner_map].astype(jnp.float32), jnp.imag(scalar_spec)[:, owner_map].astype(jnp.float32), jnp.real(spin_spec)[:, owner_map].astype(jnp.float32), jnp.imag(spin_spec)[:, owner_map].astype(jnp.float32)]
    freq = signed_freq(length)
    slot_freq = freq[owner_map]
    turns = jnp.mod(-slot_freq, 4)
    phase_real = jnp.where(turns == 0, 1.0, jnp.where(turns == 2, -1.0, 0.0)).astype(jnp.float32)
    phase_imag = jnp.where(turns == 1, 1.0, jnp.where(turns == 3, -1.0, 0.0)).astype(jnp.float32)
    outputs = []
    for degree in range(NL):
        ell = ell_index[degree]
        ell_float = ell.astype(jnp.float32)
        keep_rows = (jnp.abs(freq) <= ell).astype(jnp.float32)
        keep_slots = (jnp.abs(slot_freq) <= ell).astype(jnp.float32)
        table = deltas[:, degree, :].astype(jnp.float32)
        weight = 2.0 * math.pi / length * jnp.sqrt((2.0 * ell_float + 1.0) / (4.0 * math.pi))
        sums = []
        for plane_pos in range(4):
            spin = plane_pos // 2
            row_weights = spin_rows[:, spin, degree].astype(jnp.float32) * keep_rows
            total = jnp.einsum('k,ks->s', row_weights, table * planes[plane_pos], precision=lax.Precision.HIGHEST)
            sums.append(total * weight * keep_slots)
        coupling = prior[degree] * jnp.sqrt(ell_float * (ell_float + 1.0)) / L
        inner_real = -sums[3] - coupling * sums[0]
        inner_imag = sums[2] - coupling * sums[1]
        out_real = phase_real * inner_real - phase_imag * inner_imag
        out_imag = phase_real * inner_imag + phase_imag * inner_real
        outputs.append(jnp.stack([out_real, out_imag]))
    return jnp.stack(outputs)
```

```python
import functools
import math

import jax
import jax.numpy as jnp
import numpy as np
from jax import lax
from jax.experimental import pallas as pl
from jax.experimental.pallas import tpu as pltpu
from jax.sharding import PartitionSpec as P

F32, BF16, I16 = jnp.float32, jnp.bfloat16, jnp.int16
MESH = pl.DeviceIdType.MESH
VMEM = pl.BlockSpec(memory_space=pltpu.VMEM)
SMEM = pl.BlockSpec(memory_space=pltpu.SMEM)
NT = (((1,), (1,)), ((), ()))
TN = (((0,), (0,)), ((), ()))
LANES = 128
SPLIT = 32
CODE_TOP = 32700.0
EXTRA = 2


def halves(table):
    high = table.astype(jnp.bfloat16)
    low = (table - high.astype(np.float64)).astype(jnp.bfloat16)
    return jnp.asarray(high), jnp.asarray(low)


def turn(product, modulus):
    angle = 2.0 * np.pi / modulus * np.mod(product, modulus)
    return np.cos(angle), np.sin(angle)


def tables():
    step = np.arange(SPLIT)
    lane = np.arange(LANES)
    cos_a, sin_a = turn(np.outer(step, step), SPLIT)
    spread = np.kron(np.concatenate([cos_a, sin_a]), np.eye(8))
    cos_t, sin_t = turn(np.outer(step, lane), SPLIT * LANES)
    row_turn = np.stack([np.repeat(cos_t, 8, 0), np.repeat(sin_t, 8, 0)])
    cos_b, sin_b = turn(np.outer(lane, lane), LANES)
    wide = np.concatenate([cos_b, sin_b], 1)
    same = np.kron(np.eye(2), np.ones((SPLIT, SPLIT)))
    fold = [np.tile(np.tile(part, (2, 2)) * same, (1, 2)) for part in (cos_a, -sin_a)]
    fold = np.concatenate(fold, 1)
    cos_k, sin_k = turn(np.outer(lane, step), SPLIT * LANES)
    slot_turn = np.stack([np.tile(cos_k, (1, 4)), np.tile(sin_k, (1, 4))])
    spread_h, spread_l = halves(spread)
    wide_h, wide_l = halves(wide)
    fold_h, fold_l = halves(fold)
    return dict(
        spread_h=spread_h,
        spread_l=spread_l,
        row_turn=jnp.asarray(row_turn, F32),
        wide_h=wide_h,
        wide_l=wide_l,
        fold=jnp.concatenate([fold_h, fold_h, fold_l]),
        slot_turn=jnp.asarray(slot_turn, F32),
    )


def split2(value):
    high = value.astype(BF16)
    return high, (value - high.astype(F32)).astype(BF16)


def mm(left, right, dims=(((1,), (0,)), ((), ()))):
    return lax.dot_general(left, right, dims, preferred_element_type=F32)


def mm3(left_h, left_l, right_h, right_l, dims=(((1,), (0,)), ((), ()))):
    return mm(left_h, right_h, dims) + mm(left_h, right_l, dims) + mm(left_l, right_h, dims)


def row_kernel(x_ref, sh_ref, sl_ref, tw_ref, wh_ref, wl_ref, pos_ref, o_ref, yh_ref, yl_ref, rt_ref):
    cos_t, sin_t = tw_ref[0], tw_ref[1]

    def columns(z, i):
        return jnp.concatenate([z[8 * i : 8 * i + 8, LANES * a : LANES * (a + 1)] for a in range(SPLIT)], 0)

    def put(h, field, re_parts, im_parts):
        turned = []
        for re, im in zip(re_parts, im_parts):
            turned.append((re * cos_t + im * sin_t, im * cos_t - re * sin_t))
        for k1 in range(SPLIT):
            cut = slice(8 * k1, 8 * k1 + 8)
            re = jnp.concatenate([turned[0][0][cut], turned[1][0][cut]], 0)
            im = jnp.concatenate([turned[0][1][cut], turned[1][1][cut]], 0)
            re_h, re_l = split2(re)
            im_h, im_l = split2(im)
            top = pl.ds(k1 * LANES + field * SPLIT + 16 * h, 16)
            low = pl.ds(k1 * LANES + 64 + field * SPLIT + 16 * h, 16)
            yh_ref[top, :LANES] = re_h
            yh_ref[top, LANES:] = im_h
            yh_ref[low, :LANES] = im_h
            yh_ref[low, LANES:] = -re_h
            yl_ref[top, :LANES] = re_l
            yl_ref[top, LANES:] = im_l
            yl_ref[low, :LANES] = im_l
            yl_ref[low, LANES:] = -re_l

    for h in range(2):
        rows = pl.ds(16 * h, 16)
        v0, v1, v2, v3 = (x_ref[plane, rows, :].astype(F32) for plane in range(4))
        flat = jnp.concatenate([columns(v0, 0), columns(v0, 1)], 1).astype(BF16)
        out = mm(sh_ref[...], flat) + mm(sl_ref[...], flat)
        put(h, 0, [out[:256, :LANES], out[:256, LANES:]], [-out[256:, :LANES], -out[256:, LANES:]])
        q_re, q_im = v1 * v2, v1 * v3
        re_parts, im_parts = [], []
        for i in range(2):
            q_h, q_l = split2(jnp.concatenate([columns(q_re, i), columns(q_im, i)], 1))
            out = mm3(sh_ref[...], sl_ref[...], q_h, q_l)
            re_parts.append(out[:256, :LANES] + out[256:, LANES:])
            im_parts.append(out[:256, LANES:] - out[256:, :LANES])
        put(h, 1, re_parts, im_parts)

    def second(step, top):
        rows = pl.ds(pl.multiple_of(step * 256, 256), 256)
        out = mm3(wh_ref[...], wl_ref[...], yh_ref[rows, :], yl_ref[rows, :], NT)
        rt_ref[pl.ds(pl.multiple_of(step * 256, 256), LANES), :] = out[:, :LANES]
        rt_ref[pl.ds(pl.multiple_of(step * 256 + LANES, LANES), LANES), :] = out[:, LANES:]
        size = jnp.maximum(jnp.abs(out[:, :LANES]), jnp.abs(out[:, LANES:]))
        return jnp.maximum(top, jnp.max(size.reshape(16, 8, LANES), 0))

    top = lax.fori_loop(0, SPLIT // 2, second, jnp.zeros((8, LANES), F32))
    top = jnp.max(top, 0, keepdims=True)
    level = jnp.ceil(jnp.log2(jnp.maximum(top, 1e-30)) * 16.0 + 0.01)
    shrink = jnp.exp2(level * (-1.0 / 16.0))
    share = pos_ref.shape[0] // o_ref.shape[0]
    mark = jnp.broadcast_to(level, (EXTRA, LANES)).astype(jnp.int32).astype(I16)

    def gather(dest, _):
        for part in range(share // 16):
            base = dest * share + part * 16
            rows = [rt_ref[pl.ds(pos_ref[base + i], 1), :] for i in range(16)]
            x = jnp.concatenate(rows, 0)
            code = jnp.sqrt(jnp.abs(x) * shrink) * CODE_TOP + 0.5
            code = jnp.where(x < 0.0, -code, code).astype(jnp.int32)
            o_ref[dest, 16 * part : 16 * part + 16, :] = code.astype(I16)
        o_ref[dest, share : share + EXTRA, :] = mark
        return 0

    lax.fori_loop(0, o_ref.shape[0], gather, 0)


def row_stage(rows, position, n, share, t):
    length = rows.shape[2]
    return pl.pallas_call(
        row_kernel,
        out_shape=jax.ShapeDtypeStruct((n, share + EXTRA, LANES), I16),
        in_specs=[VMEM] * 6 + [SMEM],
        out_specs=VMEM,
        scratch_shapes=[
            pltpu.VMEM((length, 2 * LANES), BF16),
            pltpu.VMEM((length, 2 * LANES), BF16),
            pltpu.VMEM((length, LANES), F32),
        ],
        compiler_params=pltpu.CompilerParams(vmem_limit_bytes=56 * 2**20),
        name="row_stage",
    )(rows, t["spread_h"], t["spread_l"], t["row_turn"], t["wide_h"], t["wide_l"], position)


def column_kernel(
    n, send_ref, tab_ref, w_ref, hot_ref, fold_ref, st_ref, wh_ref, wl_ref, sum_ref,
    o_ref, recv_ref, t_ref, ure_ref, uim_ref, d_ref, acc_ref, ssem, rsem, lsem, share,
):
    theta, phi = lax.axis_index("theta"), lax.axis_index("phi")
    phis = lax.axis_size("phi")
    me = theta * phis + phi

    def peer(i):
        j = lax.rem(me + i, n)
        return j, {"theta": j // phis, "phi": lax.rem(j, phis)}

    barrier = pltpu.get_barrier_semaphore()

    def greet(i, _):
        pl.semaphore_signal(barrier, inc=1, device_id=peer(i)[1], device_id_type=MESH)
        return 0

    lax.fori_loop(1, n, greet, 0)
    pl.semaphore_wait(barrier, n - 1)
    own = pltpu.make_async_copy(send_ref.at[me], recv_ref.at[me], lsem)
    own.start()

    def launch(i, _):
        j, where = peer(i)
        pltpu.make_async_remote_copy(
            src_ref=send_ref.at[j],
            dst_ref=recv_ref.at[me],
            send_sem=ssem,
            recv_sem=rsem,
            device_id=where,
            device_id_type=MESH,
        ).start()
        return 0

    lax.fori_loop(1, n, launch, 0)

    def weigh(step, _):
        rows = pl.ds(pl.multiple_of(step * 512, 512), 512)
        w = mm(w_ref[rows, :], hot_ref[...])
        tab = tab_ref[rows, :].astype(F32)
        t_ref[0, rows, :] = tab * w[:, :LANES]
        t_ref[1, rows, :] = tab * w[:, LANES:]
        return 0

    lax.fori_loop(0, tab_ref.shape[0] // 512, weigh, 0)

    def fold(kl, _):
        t = jnp.concatenate([t_ref[f, pl.ds(kl, SPLIT, stride=LANES), :] for f in range(2)], 0)
        t_h, t_l = split2(t)
        v = mm(jnp.concatenate([t_h, t_l, t_h], 0), fold_ref[...], TN)
        v_re, v_im = v[:, :LANES], v[:, LANES:]
        c, s = st_ref[0, pl.ds(kl, 1), :], st_ref[1, pl.ds(kl, 1), :]
        ure_ref[pl.ds(kl, LANES, stride=LANES), :] = v_re * c + v_im * s
        uim_ref[pl.ds(kl, LANES, stride=LANES), :] = v_im * c - v_re * s
        return 0

    lax.fori_loop(0, LANES, fold, 0)

    own.wait()
    rest = pl.ds(0, n - 1)
    whole = pltpu.make_async_remote_copy(
        src_ref=send_ref.at[rest],
        dst_ref=recv_ref.at[rest],
        send_sem=ssem,
        recv_sem=rsem,
        device_id=peer(1)[1],
        device_id_type=MESH,
    )
    whole.wait_send()
    whole.wait_recv()

    def widen(tau, _):
        code = recv_ref[tau, :share, :].astype(jnp.int32).astype(F32)
        level = recv_ref[tau, share : share + EXTRA, :].astype(jnp.int32).astype(F32)[:1, :]
        grow = jnp.exp2(level * (1.0 / 16.0)) * (1.0 / CODE_TOP**2)
        d_ref[pl.ds(pl.multiple_of(tau * share, share), share), :] = code * jnp.abs(code) * grow
        return 0

    lax.fori_loop(0, n, widen, 0)
    sign = jnp.where(lax.broadcasted_iota(jnp.int32, (1, LANES), 1) < 64, 1.0, -1.0).astype(F32)

    def column(pair, _):
        cols = [d_ref[pl.ds(2 * pair + i, n, stride=share), :] for i in range(2)]
        d = jnp.concatenate(cols, 1)
        e = jnp.concatenate([pltpu.roll(x, 64, 1) * sign for x in cols], 1)
        r_h, r_l = split2(jnp.concatenate([d, e], 0))
        y = mm3(wh_ref[...], wl_ref[...], r_h, r_l)
        for i in range(2):
            y_s = y[:, i * LANES : (i + 1) * LANES]
            for j in range(4):
                row = j * share + 2 * pair + i
                rows = pl.ds(pl.multiple_of(row * LANES, LANES), LANES)
                acc_ref[pl.ds(row, 1), :] = jnp.sum(y_s * ure_ref[rows, :], 0, keepdims=True)
                acc_ref[pl.ds(LANES + row, 1), :] = jnp.sum(y_s * uim_ref[rows, :], 0, keepdims=True)
        return 0

    lax.fori_loop(0, share // 2, column, 0)
    a_h, a_m = split2(acc_ref[...])
    a_l = (acc_ref[...] - a_h.astype(F32) - a_m.astype(F32)).astype(BF16)
    o_ref[...] = mm(a_h, sum_ref[...]) + mm(a_m, sum_ref[...]) + mm(a_l, sum_ref[...])


def column_stage(send, tab, weights, t):
    n, share = send.shape[0], send.shape[1] - EXTRA
    length = tab.shape[0]
    hot = np.kron(np.eye(8), np.ones((1, share)))
    gather = np.zeros((LANES, LANES))
    gather[np.arange(LANES), np.arange(LANES) // SPLIT] = 1.0
    return pl.pallas_call(
        lambda *refs: column_kernel(n, *refs, share),
        out_shape=jax.ShapeDtypeStruct((2 * LANES, LANES), F32),
        in_specs=[VMEM] * 9,
        out_specs=VMEM,
        scratch_shapes=[
            pltpu.VMEM(send.shape, I16),
            pltpu.VMEM((2, length, LANES), F32),
            pltpu.VMEM((LANES * LANES, LANES), F32),
            pltpu.VMEM((LANES * LANES, LANES), F32),
            pltpu.VMEM((length, LANES), F32),
            pltpu.VMEM((2 * LANES, LANES), F32),
            pltpu.SemaphoreType.DMA,
            pltpu.SemaphoreType.DMA,
            pltpu.SemaphoreType.DMA,
        ],
        compiler_params=pltpu.CompilerParams(
            collective_id=0, has_side_effects=True, vmem_limit_bytes=56 * 2**20
        ),
        name="column_stage",
    )(
        send,
        tab,
        weights,
        jnp.asarray(hot, BF16),
        t["fold"],
        t["slot_turn"],
        t["wide_h"],
        t["wide_l"],
        jnp.asarray(gather, BF16),
    )


def on_device(maps, deltas, spin_rows, ell_index, owner_map, prior):
    t = tables()
    thetas, phis = lax.axis_size("theta"), lax.axis_size("phi")
    theta, phi = lax.axis_index("theta"), lax.axis_index("phi")
    length = maps.shape[2] * phis
    n = thetas * phis
    degrees = deltas.shape[1]
    share = deltas.shape[2] // phis
    rows = lax.all_to_all(maps, "phi", split_axis=1, concat_axis=2, tiled=True)
    position = (owner_map % SPLIT) * LANES + owner_map // SPLIT
    send = row_stage(rows, position, n, share, t)

    cut = deltas.reshape(deltas.shape[0], degrees, phis, share).transpose(2, 0, 1, 3)
    cut = cut.reshape(phis * deltas.shape[0], degrees * share)
    tab = lax.all_to_all(cut, "phi", split_axis=0, concat_axis=0, tiled=True)
    spins = lax.all_gather(spin_rows, "phi", axis=0, tiled=True)
    place = jnp.arange(length, dtype=jnp.int32)
    freq = jnp.where(place < length // 2, place, place - length)
    keep = jnp.abs(freq)[:, None, None] <= ell_index[None, None, :]
    weights = jnp.where(keep, spins, 0).astype(BF16).reshape(length, 2 * degrees)
    sums = column_stage(send, tab, weights, t)

    sums = sums[:, :4].reshape(2, degrees, share, 4).transpose(0, 3, 1, 2)
    scalar_real, scalar_imag = sums[0, 0] - sums[1, 2], sums[0, 2] + sums[1, 0]
    spin_real, spin_imag = sums[0, 1] - sums[1, 3], sums[0, 3] + sums[1, 1]
    ids = lax.dynamic_slice_in_dim(owner_map, (theta * phis + phi) * share, share)
    slot_freq = jnp.where(ids < length // 2, ids, ids - length)
    ell = ell_index.astype(F32)
    weight = 2.0 * math.pi / length * jnp.sqrt((2.0 * ell + 1.0) / (4.0 * math.pi)) / length
    keep = jnp.where(jnp.abs(slot_freq)[None, :] <= ell_index[:, None], weight[:, None], 0.0)
    coupling = (prior * jnp.sqrt(ell * (ell + 1.0)) / (length // 2))[:, None]
    inner_real = (-spin_imag - coupling * scalar_real) * keep
    inner_imag = (spin_real - coupling * scalar_imag) * keep
    turns = jnp.mod(-slot_freq, 4)
    phase_real = jnp.where(turns == 0, 1.0, jnp.where(turns == 2, -1.0, 0.0)).astype(F32)[None, :]
    phase_imag = jnp.where(turns == 1, 1.0, jnp.where(turns == 3, -1.0, 0.0)).astype(F32)[None, :]
    out_real = phase_real * inner_real - phase_imag * inner_imag
    out_imag = phase_real * inner_imag + phase_imag * inner_real
    return jnp.stack([out_real, out_imag], axis=1)


def solution(mesh):
    placed = (
        P("grp", "theta", "phi"),
        P("phi", None, "theta"),
        P("phi", None, None),
        P(),
        P(),
        P(),
    )
    return jax.shard_map(
        on_device,
        mesh=mesh,
        in_specs=placed,
        out_specs=P("grp", None, ("theta", "phi")),
        check_vma=False,
    )
```

```python
import math

import jax
import jax.numpy as jnp
import numpy as np
from jax import lax
from jax.experimental import pallas as pl
from jax.experimental.pallas import tpu as pltpu
from jax.sharding import PartitionSpec as P

F32, BF16, I16 = jnp.float32, jnp.bfloat16, jnp.int16
MESH = pl.DeviceIdType.MESH
VMEM = pl.BlockSpec(memory_space=pltpu.VMEM)
SMEM = pl.BlockSpec(memory_space=pltpu.SMEM)
ANY = pl.BlockSpec(memory_space=pl.ANY)
NN = (((1,), (0,)), ((), ()))
NT = (((1,), (1,)), ((), ()))
TN = (((0,), (0,)), ((), ()))
LANES = 128
SPLIT = 32
HALF = LANES // 2
GROUP = 32
CODE_TOP = 32700.0


def halves(table):
    high = table.astype(jnp.bfloat16)
    low = (table - high.astype(np.float64)).astype(jnp.bfloat16)
    return jnp.asarray(high), jnp.asarray(low)


def turn(product, modulus):
    angle = 2.0 * np.pi / modulus * np.mod(product, modulus)
    return np.cos(angle), np.sin(angle)


def tables():
    step = np.arange(SPLIT)
    lane = np.arange(LANES)
    cos_a, sin_a = turn(np.outer(step, step), SPLIT)
    spread_h, spread_l = halves(np.kron(np.concatenate([cos_a, sin_a]), np.eye(8)))
    cos_t, sin_t = turn(np.outer(step, lane), SPLIT * LANES)
    row_turn = np.stack([np.repeat(cos_t, 8, 0), np.repeat(sin_t, 8, 0)])
    cos_b, sin_b = turn(np.outer(lane, lane), LANES)
    wide = np.concatenate([cos_b, sin_b], 1)
    wide_h, wide_l = halves(wide)
    fold_h, fold_l = halves(np.concatenate([np.kron(np.eye(2), cos_a), np.kron(np.eye(2), -sin_a)], 1))
    cos_k, sin_k = turn(np.outer(lane, step), SPLIT * LANES)
    slot_turn = np.stack([np.tile(cos_k, (1, 4)), np.concatenate([sin_k, sin_k, -sin_k, -sin_k], 1)])
    gather = np.zeros((LANES, LANES))
    gather[lane, lane // SPLIT] = 1.0
    return (
        spread_h,
        spread_l,
        jnp.asarray(row_turn, F32),
        wide_h,
        wide_l,
        jnp.asarray(wide, F32),
        jnp.concatenate([fold_h, fold_h, fold_l]),
        jnp.asarray(slot_turn, F32),
        jnp.asarray(gather, BF16),
    )


def split2(value):
    high = value.astype(BF16)
    return high, (value - high.astype(F32)).astype(BF16)


def mm(left, right, dims=NN):
    return lax.dot_general(left, right, dims, preferred_element_type=F32)


def mm3(left_h, left_l, right_h, right_l, dims=NN):
    return mm(left_h, right_h, dims) + mm(left_h, right_l, dims) + mm(left_l, right_h, dims)


def row_spectra(x_ref, sh_ref, sl_ref, tw_ref, wh_ref, wl_ref, yh_ref, yl_ref, rt_ref):
    cos_t, sin_t = tw_ref[0], tw_ref[1]

    def columns(z, i):
        return jnp.concatenate([z[8 * i : 8 * i + 8, LANES * a : LANES * (a + 1)] for a in range(SPLIT)], 0)

    def put(h, field, re_parts, im_parts):
        turned = []
        for re, im in zip(re_parts, im_parts):
            turned.append((re * cos_t + im * sin_t, im * cos_t - re * sin_t))
        for k1 in range(SPLIT):
            cut = slice(8 * k1, 8 * k1 + 8)
            re = jnp.concatenate([turned[0][0][cut], turned[1][0][cut]], 0)
            im = jnp.concatenate([turned[0][1][cut], turned[1][1][cut]], 0)
            re_h, re_l = split2(re)
            im_h, im_l = split2(im)
            top = pl.ds(k1 * LANES + field * SPLIT + 16 * h, 16)
            low = pl.ds(k1 * LANES + HALF + field * SPLIT + 16 * h, 16)
            yh_ref[top, :LANES] = re_h
            yh_ref[top, LANES:] = im_h
            yh_ref[low, :LANES] = im_h
            yh_ref[low, LANES:] = -re_h
            yl_ref[top, :LANES] = re_l
            yl_ref[top, LANES:] = im_l
            yl_ref[low, :LANES] = im_l
            yl_ref[low, LANES:] = -re_l

    row_id = lax.broadcasted_iota(jnp.int32, (16, LANES), 0)
    lane_id = lax.broadcasted_iota(jnp.int32, (16, LANES), 1)
    bound = jnp.zeros((1, LANES), F32)
    for h in range(2):
        rows = pl.ds(16 * h, 16)
        v0, v1, v2, v3 = (x_ref[plane, rows, :].astype(F32) for plane in range(4))
        q_re, q_im = v1 * v2, v1 * v3
        sizes = jnp.sum(jnp.abs(v0), 1, keepdims=True), jnp.sum(jnp.abs(q_re) + jnp.abs(q_im), 1, keepdims=True)
        for field in range(2):
            here = lane_id % HALF == row_id + (field * SPLIT + 16 * h)
            bound = bound + jnp.sum(jnp.where(here, sizes[field], 0.0), 0, keepdims=True)
        flat = jnp.concatenate([columns(v0, 0), columns(v0, 1)], 1).astype(BF16)
        out = mm(sh_ref[...], flat) + mm(sl_ref[...], flat)
        put(h, 0, [out[:256, :LANES], out[:256, LANES:]], [-out[256:, :LANES], -out[256:, LANES:]])
        re_parts, im_parts = [], []
        for i in range(2):
            q_h, q_l = split2(jnp.concatenate([columns(q_re, i), columns(q_im, i)], 1))
            out = mm3(sh_ref[...], sl_ref[...], q_h, q_l)
            re_parts.append(out[:256, :LANES] + out[256:, LANES:])
            im_parts.append(out[:256, LANES:] - out[256:, :LANES])
        put(h, 1, re_parts, im_parts)

    def second(step, _):
        rows = pl.ds(pl.multiple_of(step * 256, 256), 256)
        out = mm3(wh_ref[...], wl_ref[...], yh_ref[rows, :], yl_ref[rows, :], NT)
        rt_ref[pl.ds(pl.multiple_of(step * 256, 256), LANES), :] = out[:, :LANES]
        rt_ref[pl.ds(pl.multiple_of(step * 256 + LANES, LANES), LANES), :] = out[:, LANES:]
        return 0

    lax.fori_loop(0, SPLIT // 2, second, 0)
    return jnp.maximum(bound, 1e-30)


def kernel(
    maps_ref, delta_ref, spin_ref, pos_ref, sh_ref, sl_ref, tw_ref, wh_ref, wl_ref, wide_ref, fold_ref, st_ref, sum_ref,
    o_ref,
    x_ref, yh_ref, yl_ref, rt_ref, send_ref, recv_ref, bound_ref, bounds_ref, tab_ref, w_ref, t_ref, wt_ref,
    mine_ref, h_ref, d_ref, acc_ref, near_sem, far_sem, out_sem, ssem, rsem, bsem, brsem,
):
    theta, phi = lax.axis_index("theta"), lax.axis_index("phi")
    phis = lax.axis_size("phi")
    n, share = recv_ref.shape[0], recv_ref.shape[1]
    me = theta * phis + phi
    other = phis - 1 - phi
    half = maps_ref.shape[2]
    here = pl.ds(pl.multiple_of(phi * half, half), half)

    def peer(i):
        j = lax.rem(me + i, n)
        return j, {"theta": j // phis, "phi": lax.rem(j, phis)}

    def cut(whose):
        return pl.ds(pl.multiple_of(whose * share, share), share)

    pieces = (
        (lambda whose: maps_ref.at[:, cut(whose), :], x_ref.at[:, :, here]),
        (lambda whose: delta_ref.at[:, cut(whose), :], tab_ref.at[:, :, here]),
        (lambda whose: spin_ref, w_ref.at[:, here]),
    )
    near = [pltpu.make_async_copy(src(phi), dst, near_sem.at[k]) for k, (src, dst) in enumerate(pieces)]
    far = [
        pltpu.make_async_remote_copy(
            src_ref=src(other),
            dst_ref=dst,
            send_sem=out_sem.at[k],
            recv_sem=far_sem.at[k],
            device_id={"phi": other},
            device_id_type=MESH,
        )
        for k, (src, dst) in enumerate(pieces)
    ]
    near[0].start()

    barrier = pltpu.get_barrier_semaphore()

    def greet(i, _):
        pl.semaphore_signal(barrier, inc=1, device_id=peer(i)[1], device_id_type=MESH)
        return 0

    lax.fori_loop(1, n, greet, 0)
    pl.semaphore_wait(barrier, n - 1)
    for copy in far:
        copy.start()
    for copy in near[1:]:
        copy.start()
    near[0].wait()
    far[0].wait()

    bound = row_spectra(x_ref, sh_ref, sl_ref, tw_ref, wh_ref, wl_ref, yh_ref, yl_ref, rt_ref)
    bound_ref[...] = bound
    bounds_ref[0] = bound
    shrink = 1.0 / bound

    def tell(i):
        return pltpu.make_async_remote_copy(
            src_ref=bound_ref,
            dst_ref=bounds_ref.at[i],
            send_sem=bsem,
            recv_sem=brsem,
            device_id=peer(i)[1],
            device_id_type=MESH,
        )

    def encoded(dest, target, slot):
        for part in range(share // 16):
            base = dest * share + part * 16
            rows = [rt_ref[pl.ds(pos_ref[base + i], 1), :] for i in range(16)]
            x = jnp.concatenate(rows, 0)
            code = jnp.sqrt(jnp.abs(x) * shrink) * CODE_TOP + 0.5
            code = jnp.where(x < 0.0, -code, code).astype(jnp.int32)
            target[slot, 16 * part : 16 * part + 16, :] = code.astype(I16)

    def post(i):
        pltpu.make_async_remote_copy(
            src_ref=send_ref.at[i],
            dst_ref=recv_ref.at[i],
            send_sem=ssem,
            recv_sem=rsem.at[i // GROUP],
            device_id=peer(i)[1],
            device_id_type=MESH,
        ).start()

    def tell_all(i, _):
        tell(i).start()
        return 0

    lax.fori_loop(1, n, tell_all, 0)
    encoded(peer(1)[0], send_ref, 1)

    def ship(i, _):
        post(i - 1)
        encoded(peer(i)[0], send_ref, i)
        return 0

    lax.fori_loop(2, n, ship, 0)
    encoded(me, recv_ref, 0)
    post(n - 1)

    for copy in near[1:]:
        copy.wait()
    for copy in far[1:]:
        copy.wait()
    degrees = tab_ref.shape[0]

    def arrange(kh, _):
        lanes = pl.ds(pl.multiple_of(kh * LANES, LANES), LANES)
        for j in range(degrees):
            rows = pl.ds(pl.multiple_of(kh * LANES + j * share, share), share)
            t_ref[rows, :] = tab_ref[j, :, lanes].astype(F32)
        wt_ref[pl.ds(pl.multiple_of(kh * 8, 8), 8), :] = w_ref[:, lanes]
        return 0

    lax.fori_loop(0, SPLIT, arrange, 0)

    def order(i, _):
        mine_ref[pl.ds(i, 1), :] = wide_ref[pl.ds(lax.rem(me - i + n, n), 1), :]
        return 0

    lax.fori_loop(0, n, order, 0)
    lane_id = lax.broadcasted_iota(jnp.int32, (1, LANES), 1)
    first = lane_id < HALF
    sign = jnp.where(first, 1.0, -1.0).astype(F32)

    def fold(pair, _):
        tops = []
        for i in range(2):
            js = 2 * pair + i
            j = js // share
            t = t_ref[pl.ds(js, SPLIT, stride=LANES), :]
            both = [t * wt_ref[pl.ds(f * degrees + j, SPLIT, stride=8), :] for f in range(2)]
            t_h, t_l = split2(jnp.concatenate(both, 0))
            v = mm(jnp.concatenate([t_h, t_l, t_h], 0), fold_ref[...], TN)
            tops.append(v * st_ref[0] + pltpu.roll(v, HALF, 1) * st_ref[1])
        lows = [pltpu.roll(u, HALF, 1) * sign for u in tops]
        r_h, r_l = split2(jnp.concatenate([jnp.concatenate(tops, 1), jnp.concatenate(lows, 1)], 0))
        m_h, m_l = split2(mine_ref[...])
        out = mm3(m_h, m_l, r_h, r_l)
        for i in range(2):
            g = out[:, i * LANES : (i + 1) * LANES]
            back = pltpu.roll(g, HALF, 1)
            rows = pl.ds(pl.multiple_of((2 * pair + i) * LANES, LANES), LANES)
            h_ref[rows, :LANES] = jnp.where(first, g, back)
            h_ref[rows, LANES:] = jnp.where(first, back, g)
        return 0

    lax.fori_loop(0, LANES // 2, fold, 0)
    acc_ref[...] = jnp.zeros_like(acc_ref)

    rest = pl.ds(1, n - 1)
    bounds = pltpu.make_async_remote_copy(
        src_ref=bounds_ref.at[rest],
        dst_ref=bounds_ref.at[rest],
        send_sem=bsem,
        recv_sem=brsem,
        device_id=peer(1)[1],
        device_id_type=MESH,
    )
    bounds.wait_send()
    bounds.wait_recv()
    for group in range(n // GROUP):
        begin = group * GROUP
        part = pl.ds(max(begin, 1), GROUP - (begin == 0))
        pltpu.make_async_remote_copy(
            src_ref=send_ref.at[part],
            dst_ref=recv_ref.at[part],
            send_sem=ssem,
            recv_sem=rsem.at[group],
            device_id=peer(1)[1],
            device_id_type=MESH,
        ).wait_recv()

        def widen(k, _):
            slot = begin + k
            code = recv_ref[slot].astype(jnp.int32).astype(F32)
            grow = bounds_ref[slot] * (1.0 / CODE_TOP**2)
            d_ref[pl.ds(pl.multiple_of(k * share, share), share), :] = code * jnp.abs(code) * grow
            return 0

        lax.fori_loop(0, GROUP, widen, 0)

        def gain(s, _):
            d = d_ref[pl.ds(s, GROUP, stride=share), :]
            for j in range(degrees):
                row = j * share + s
                rows = pl.ds(pl.multiple_of(row * LANES + begin, GROUP), GROUP)
                for k in range(2):
                    sums = jnp.sum((d * h_ref[rows, k * LANES : (k + 1) * LANES]).reshape(-1, 8, LANES), 0)
                    place = pl.ds(pl.multiple_of((k * LANES + row) * 8, 8), 8)
                    acc_ref[place, :] = acc_ref[place, :] + sums
            return 0

        lax.fori_loop(0, share, gain, 0)

    total = jnp.sum(acc_ref[...].reshape(2 * LANES, 8, LANES), 1)
    a_h, a_m = split2(total)
    a_l = (total - a_h.astype(F32) - a_m.astype(F32)).astype(BF16)
    o_ref[...] = mm(a_h, sum_ref[...]) + mm(a_m, sum_ref[...]) + mm(a_l, sum_ref[...])
    sent = pl.ds(1, n - 1)
    pltpu.make_async_remote_copy(
        src_ref=send_ref.at[sent],
        dst_ref=recv_ref.at[sent],
        send_sem=ssem,
        recv_sem=rsem.at[0],
        device_id=peer(1)[1],
        device_id_type=MESH,
    ).wait_send()


def sums_of(maps, deltas, spins, position, n):
    degrees, slots, half = deltas.shape
    share = slots * half // position.shape[0]
    length = position.shape[0]
    dma = pltpu.SemaphoreType.DMA
    return pl.pallas_call(
        kernel,
        out_shape=jax.ShapeDtypeStruct((2 * LANES, LANES), F32),
        in_specs=[ANY] * 3 + [SMEM] + [VMEM] * 9,
        out_specs=VMEM,
        scratch_shapes=[
            pltpu.VMEM((4, SPLIT, length), BF16),
            pltpu.VMEM((length, 2 * LANES), BF16),
            pltpu.VMEM((length, 2 * LANES), BF16),
            pltpu.VMEM((length, LANES), F32),
            pltpu.VMEM((n, share, LANES), I16),
            pltpu.VMEM((n, share, LANES), I16),
            pltpu.VMEM((1, LANES), F32),
            pltpu.VMEM((n, 1, LANES), F32),
            pltpu.VMEM((degrees, share, length), BF16),
            pltpu.VMEM((2 * degrees, length), F32),
            pltpu.VMEM((length, LANES), F32),
            pltpu.VMEM((SPLIT * 2 * degrees, LANES), F32),
            pltpu.VMEM((n, 2 * LANES), F32),
            pltpu.VMEM((LANES * LANES, 2 * LANES), F32),
            pltpu.VMEM((GROUP * share, LANES), F32),
            pltpu.VMEM((2 * LANES * 8, LANES), F32),
            dma((3,)),
            dma((3,)),
            dma((3,)),
            dma,
            dma((n // GROUP,)),
            dma,
            dma,
        ],
        compiler_params=pltpu.CompilerParams(
            collective_id=0, has_side_effects=True, vmem_limit_bytes=56 * 2**20
        ),
        name="coefficient_sums",
    )(maps, deltas, spins, position, *tables())


def on_device(maps, deltas, spin_rows, ell_index, owner_map, prior):
    thetas, phis = lax.axis_size("theta"), lax.axis_size("phi")
    theta, phi = lax.axis_index("theta"), lax.axis_index("phi")
    half = maps.shape[2]
    length = half * phis
    n = thetas * phis
    degrees = deltas.shape[1]
    share = deltas.shape[2] // phis
    position = (owner_map % SPLIT) * LANES + owner_map // SPLIT
    place = phi * half + jnp.arange(half, dtype=jnp.int32)
    freq = jnp.where(place < length // 2, place, place - length)
    keep = jnp.abs(freq)[None, None, :] <= ell_index[None, :, None]
    spins = jnp.where(keep, spin_rows.transpose(1, 2, 0).astype(F32), 0.0).reshape(2 * degrees, half)
    sums = sums_of(maps, deltas.transpose(1, 2, 0), spins, position, n)

    sums = sums[:, :4].reshape(2, degrees, share, 4).transpose(0, 3, 1, 2)
    scalar_real, scalar_imag = sums[0, 0] - sums[1, 2], sums[0, 2] + sums[1, 0]
    spin_real, spin_imag = sums[0, 1] - sums[1, 3], sums[0, 3] + sums[1, 1]
    ids = lax.dynamic_slice_in_dim(owner_map, (theta * phis + phi) * share, share)
    slot_freq = jnp.where(ids < length // 2, ids, ids - length)
    ell = ell_index.astype(F32)
    weight = 2.0 * math.pi / length * jnp.sqrt((2.0 * ell + 1.0) / (4.0 * math.pi)) / length
    keep = jnp.where(jnp.abs(slot_freq)[None, :] <= ell_index[:, None], weight[:, None], 0.0)
    coupling = (prior * jnp.sqrt(ell * (ell + 1.0)) / (length // 2))[:, None]
    inner_real = (-spin_imag - coupling * scalar_real) * keep
    inner_imag = (spin_real - coupling * scalar_imag) * keep
    turns = jnp.mod(-slot_freq, 4)
    phase_real = jnp.where(turns == 0, 1.0, jnp.where(turns == 2, -1.0, 0.0)).astype(F32)[None, :]
    phase_imag = jnp.where(turns == 1, 1.0, jnp.where(turns == 3, -1.0, 0.0)).astype(F32)[None, :]
    out_real = phase_real * inner_real - phase_imag * inner_imag
    out_imag = phase_real * inner_imag + phase_imag * inner_real
    return jnp.stack([out_real, out_imag], axis=1)


def solution(mesh):
    placed = (
        P("grp", "theta", "phi"),
        P("phi", None, "theta"),
        P("phi", None, None),
        P(),
        P(),
        P(),
    )
    return jax.shard_map(
        on_device,
        mesh=mesh,
        in_specs=placed,
        out_specs=P("grp", None, ("theta", "phi")),
        check_vma=False,
    )
```

```python
import math

import jax
import jax.numpy as jnp
import numpy as np
from jax import lax
from jax.experimental import pallas as pl
from jax.experimental.pallas import tpu as pltpu
from jax.sharding import PartitionSpec as P

F32, BF16, I16 = jnp.float32, jnp.bfloat16, jnp.int16
MESH = pl.DeviceIdType.MESH
VMEM = pl.BlockSpec(memory_space=pltpu.VMEM)
SMEM = pl.BlockSpec(memory_space=pltpu.SMEM)
ANY = pl.BlockSpec(memory_space=pl.ANY)
NN = (((1,), (0,)), ((), ()))
NT = (((1,), (1,)), ((), ()))
TN = (((0,), (0,)), ((), ()))
LANES = 128
SPLIT = 32
HALF = LANES // 2
GROUP = 32
UNROLL = 2
CODE_TOP = 32700.0


def halves(table):
    high = table.astype(jnp.bfloat16)
    low = (table - high.astype(np.float64)).astype(jnp.bfloat16)
    return jnp.asarray(high), jnp.asarray(low)


def turn(product, modulus):
    angle = 2.0 * np.pi / modulus * np.mod(product, modulus)
    return np.cos(angle), np.sin(angle)


def tables():
    step = np.arange(SPLIT)
    lane = np.arange(LANES)
    cos_a, sin_a = turn(np.outer(step, step), SPLIT)
    spread_h, spread_l = halves(np.kron(np.concatenate([cos_a, sin_a]), np.eye(8)))
    cos_t, sin_t = turn(np.outer(step, lane), SPLIT * LANES)
    row_turn = np.stack([np.repeat(cos_t, 8, 0), np.repeat(sin_t, 8, 0)])
    cos_b, sin_b = turn(np.outer(lane, lane), LANES)
    wide = np.concatenate([cos_b, sin_b], 1)
    wide_h, wide_l = halves(wide)
    fold_h, fold_l = halves(np.concatenate([np.kron(np.eye(2), cos_a), np.kron(np.eye(2), -sin_a)], 1))
    cos_k, sin_k = turn(np.outer(lane, step), SPLIT * LANES)
    slot_turn = np.stack([np.tile(cos_k, (1, 4)), np.concatenate([sin_k, sin_k, -sin_k, -sin_k], 1)])
    gather = np.zeros((8, LANES))
    gather[lane // SPLIT, lane] = 1.0
    return (
        spread_h,
        spread_l,
        jnp.asarray(row_turn, F32),
        wide_h,
        wide_l,
        jnp.asarray(wide, F32),
        jnp.concatenate([fold_h, fold_h, fold_l]),
        jnp.asarray(slot_turn, F32),
        jnp.asarray(gather, BF16),
    )


def split2(value):
    high = value.astype(BF16)
    return high, (value - high.astype(F32)).astype(BF16)


def mm(left, right, dims=NN):
    return lax.dot_general(left, right, dims, preferred_element_type=F32)


def mm3(left_h, left_l, right_h, right_l, dims=NN):
    return mm(left_h, right_h, dims) + mm(left_h, right_l, dims) + mm(left_l, right_h, dims)


def row_spectra(x_ref, sh_ref, sl_ref, tw_ref, wh_ref, wl_ref, yh_ref, yl_ref, rt_ref):
    cos_t, sin_t = tw_ref[0], tw_ref[1]

    def columns(z, i):
        return jnp.concatenate([z[8 * i : 8 * i + 8, LANES * a : LANES * (a + 1)] for a in range(SPLIT)], 0)

    def put(h, field, re_parts, im_parts):
        turned = []
        for re, im in zip(re_parts, im_parts):
            turned.append((re * cos_t + im * sin_t, im * cos_t - re * sin_t))
        for k1 in range(SPLIT):
            cut = slice(8 * k1, 8 * k1 + 8)
            re = jnp.concatenate([turned[0][0][cut], turned[1][0][cut]], 0)
            im = jnp.concatenate([turned[0][1][cut], turned[1][1][cut]], 0)
            re_h, re_l = split2(re)
            im_h, im_l = split2(im)
            top = pl.ds(k1 * LANES + field * SPLIT + 16 * h, 16)
            low = pl.ds(k1 * LANES + HALF + field * SPLIT + 16 * h, 16)
            yh_ref[top, :LANES] = re_h
            yh_ref[top, LANES:] = im_h
            yh_ref[low, :LANES] = im_h
            yh_ref[low, LANES:] = -re_h
            yl_ref[top, :LANES] = re_l
            yl_ref[top, LANES:] = im_l
            yl_ref[low, :LANES] = im_l
            yl_ref[low, LANES:] = -re_l

    row_id = lax.broadcasted_iota(jnp.int32, (16, LANES), 0)
    lane_id = lax.broadcasted_iota(jnp.int32, (16, LANES), 1)
    bound = jnp.zeros((1, LANES), F32)
    for h in range(2):
        rows = pl.ds(16 * h, 16)
        v0, v1, v2, v3 = (x_ref[plane, rows, :].astype(F32) for plane in range(4))
        q_re, q_im = v1 * v2, v1 * v3
        sizes = jnp.sum(jnp.abs(v0), 1, keepdims=True), jnp.sum(jnp.abs(q_re) + jnp.abs(q_im), 1, keepdims=True)
        for field in range(2):
            here = lane_id % HALF == row_id + (field * SPLIT + 16 * h)
            bound = bound + jnp.sum(jnp.where(here, sizes[field], 0.0), 0, keepdims=True)
        flat = jnp.concatenate([columns(v0, 0), columns(v0, 1)], 1).astype(BF16)
        out = mm(sh_ref[...], flat) + mm(sl_ref[...], flat)
        put(h, 0, [out[:256, :LANES], out[:256, LANES:]], [-out[256:, :LANES], -out[256:, LANES:]])
        re_parts, im_parts = [], []
        for i in range(2):
            q_h, q_l = split2(jnp.concatenate([columns(q_re, i), columns(q_im, i)], 1))
            out = mm3(sh_ref[...], sl_ref[...], q_h, q_l)
            re_parts.append(out[:256, :LANES] + out[256:, LANES:])
            im_parts.append(out[:256, LANES:] - out[256:, :LANES])
        put(h, 1, re_parts, im_parts)

    def second(step, _):
        rows = pl.ds(pl.multiple_of(step * 256, 256), 256)
        out = mm3(wh_ref[...], wl_ref[...], yh_ref[rows, :], yl_ref[rows, :], NT)
        rt_ref[pl.ds(pl.multiple_of(step * 256, 256), LANES), :] = out[:, :LANES]
        rt_ref[pl.ds(pl.multiple_of(step * 256 + LANES, LANES), LANES), :] = out[:, LANES:]
        return 0

    lax.fori_loop(0, SPLIT // 2, second, 0)
    return jnp.maximum(bound, 1e-30)


def kernel(
    maps_ref, delta_ref, spin_ref, pos_ref, ell_ref, sh_ref, sl_ref, tw_ref, wh_ref, wl_ref, wide_ref, fold_ref, st_ref, sum_ref,
    o_ref,
    x_ref, yh_ref, yl_ref, rt_ref, send_ref, recv_ref, bound_ref, bounds_ref, tab_ref, w_ref, t_ref, wt_ref,
    mine_ref, h_ref, d_ref, acc_ref, near_sem, far_sem, out_sem, ssem, rsem, bsem, brsem,
):
    theta, phi = lax.axis_index("theta"), lax.axis_index("phi")
    phis = lax.axis_size("phi")
    n, share = recv_ref.shape[0], recv_ref.shape[1]
    me = theta * phis + phi
    other = phis - 1 - phi
    half = maps_ref.shape[2]
    here = pl.ds(pl.multiple_of(phi * half, half), half)

    def peer(i):
        j = lax.rem(me + i, n)
        return j, {"theta": lax.div(j, phis), "phi": lax.rem(j, phis)}

    def cut(whose):
        return pl.ds(pl.multiple_of(whose * share, share), share)

    pieces = (
        (lambda whose: maps_ref.at[:, cut(whose), :], x_ref.at[:, :, here]),
        (lambda whose: delta_ref.at[:, cut(whose), :], tab_ref.at[:, :, here]),
        (lambda whose: spin_ref, w_ref.at[:, :, here]),
    )
    near = [pltpu.make_async_copy(src(phi), dst, near_sem.at[k]) for k, (src, dst) in enumerate(pieces)]
    far = [
        pltpu.make_async_remote_copy(
            src_ref=src(other),
            dst_ref=dst,
            send_sem=out_sem.at[k],
            recv_sem=far_sem.at[k],
            device_id={"phi": other},
            device_id_type=MESH,
        )
        for k, (src, dst) in enumerate(pieces)
    ]
    near[0].start()

    barrier = pltpu.get_barrier_semaphore()

    def greet(i):
        pl.semaphore_signal(barrier, inc=1, device_id=peer(i)[1], device_id_type=MESH)

    def greet_some(step, _):
        for k in range(7):
            greet(1 + step * 7 + k)
        return 0

    lax.fori_loop(0, (n - 1) // 7, greet_some, 0)
    for k in range(1 + (n - 1) // 7 * 7, n):
        greet(k)
    pl.semaphore_wait(barrier, n - 1)
    for copy in far:
        copy.start()
    for copy in near[1:]:
        copy.start()
    near[0].wait()
    far[0].wait()

    bound = row_spectra(x_ref, sh_ref, sl_ref, tw_ref, wh_ref, wl_ref, yh_ref, yl_ref, rt_ref)
    bound_ref[...] = bound
    bounds_ref[0] = bound
    shrink = 1.0 / bound

    def encoded(dest, target, slot):
        for part in range(share // 16):
            base = dest * share + part * 16
            rows = [rt_ref[pl.ds(pos_ref[base + i], 1), :] for i in range(16)]
            x = jnp.concatenate(rows, 0)
            code = jnp.sqrt(jnp.abs(x) * shrink) * CODE_TOP + 0.5
            code = jnp.where(x < 0.0, -code, code).astype(jnp.int32)
            target[slot, 16 * part : 16 * part + 16, :] = code.astype(I16)

    def post(i):
        where = peer(i)[1]
        pltpu.make_async_remote_copy(
            src_ref=bound_ref,
            dst_ref=bounds_ref.at[i],
            send_sem=bsem,
            recv_sem=brsem,
            device_id=where,
            device_id_type=MESH,
        ).start()
        pltpu.make_async_remote_copy(
            src_ref=send_ref.at[i],
            dst_ref=recv_ref.at[i],
            send_sem=ssem,
            recv_sem=rsem.at[i // GROUP],
            device_id=where,
            device_id_type=MESH,
        ).start()

    def fill(i):
        encoded(peer(i)[0], send_ref, i)

    middle = n // 2
    fill(middle)
    fill(1)
    fill(middle + 1)
    post(middle)

    def ship(step, _):
        base = 2 + step * UNROLL
        for k in range(UNROLL):
            i = base + k
            post(i - 1)
            post(middle + i - 1)
            fill(i)
            fill(middle + i)
        return 0

    lax.fori_loop(0, (middle - 2) // UNROLL, ship, 0)
    post(middle - 1)
    post(n - 1)
    encoded(me, recv_ref, 0)

    for copy in near[1:]:
        copy.wait()
    for copy in far[1:]:
        copy.wait()
    degrees, length = tab_ref.shape[0], tab_ref.shape[2]

    def arrange(kh, _):
        lanes = pl.ds(pl.multiple_of(kh * LANES, LANES), LANES)
        for j in range(degrees):
            rows = pl.ds(pl.multiple_of(kh * LANES + j * share, share), share)
            t_ref[rows, :] = tab_ref[j, :, lanes].astype(F32)
        w = jnp.concatenate([w_ref[f, :, lanes].astype(F32) for f in range(2)], 0)
        place = kh * LANES + lax.broadcasted_iota(jnp.int32, w.shape, 1)
        freq = jnp.where(place < length // 2, place, place - length)
        row = lax.broadcasted_iota(jnp.int32, w.shape, 0) % degrees
        ell = jnp.zeros(w.shape, jnp.int32)
        for j in range(degrees):
            ell = jnp.where(row == j, ell_ref[j], ell)
        wt_ref[pl.ds(pl.multiple_of(kh * 8, 8), 8), :] = jnp.where(jnp.abs(freq) <= ell, w, 0.0)
        return 0

    lax.fori_loop(0, SPLIT, arrange, 0)

    def order(i, _):
        mine_ref[pl.ds(i, 1), :] = wide_ref[pl.ds((me - i + n) % n, 1), :]
        return 0

    lax.fori_loop(0, n, order, 0)
    lane_id = lax.broadcasted_iota(jnp.int32, (1, LANES), 1)
    first = lane_id < HALF
    sign = jnp.where(first, 1.0, -1.0).astype(F32)

    def fold(pair, _):
        tops = []
        for i in range(2):
            js = 2 * pair + i
            j = js // share
            t = t_ref[pl.ds(js, SPLIT, stride=LANES), :]
            both = [t * wt_ref[pl.ds(f * degrees + j, SPLIT, stride=8), :] for f in range(2)]
            t_h, t_l = split2(jnp.concatenate(both, 0))
            v = mm(jnp.concatenate([t_h, t_l, t_h], 0), fold_ref[...], TN)
            tops.append(v * st_ref[0] + pltpu.roll(v, HALF, 1) * st_ref[1])
        lows = [pltpu.roll(u, HALF, 1) * sign for u in tops]
        r_h, r_l = split2(jnp.concatenate([jnp.concatenate(tops, 1), jnp.concatenate(lows, 1)], 0))
        m_h, m_l = split2(mine_ref[...])
        out = mm3(m_h, m_l, r_h, r_l)
        for i in range(2):
            g = out[:, i * LANES : (i + 1) * LANES]
            back = pltpu.roll(g, HALF, 1)
            rows = pl.ds(pl.multiple_of((2 * pair + i) * LANES, LANES), LANES)
            h_ref[rows, :LANES] = jnp.where(first, g, back)
            h_ref[rows, LANES:] = jnp.where(first, back, g)
        return 0

    lax.fori_loop(0, LANES // 2, fold, 0)
    acc_ref[...] = jnp.zeros_like(acc_ref)

    rest = pl.ds(1, n - 1)
    bounds = pltpu.make_async_remote_copy(
        src_ref=bounds_ref.at[rest],
        dst_ref=bounds_ref.at[rest],
        send_sem=bsem,
        recv_sem=brsem,
        device_id=peer(1)[1],
        device_id_type=MESH,
    )
    bounds.wait_send()
    bounds.wait_recv()
    groups = n // GROUP
    for group in [k // 2 + k % 2 * (groups // 2) for k in range(groups)]:
        begin = group * GROUP
        part = pl.ds(max(begin, 1), GROUP - (begin == 0))
        pltpu.make_async_remote_copy(
            src_ref=send_ref.at[part],
            dst_ref=recv_ref.at[part],
            send_sem=ssem,
            recv_sem=rsem.at[group],
            device_id=peer(1)[1],
            device_id_type=MESH,
        ).wait_recv()

        def widen(k, _):
            slot = begin + k
            code = recv_ref[slot].astype(jnp.int32).astype(F32)
            grow = bounds_ref[slot] * (1.0 / CODE_TOP**2)
            d_ref[pl.ds(pl.multiple_of(k * share, share), share), :] = code * jnp.abs(code) * grow
            return 0

        lax.fori_loop(0, GROUP, widen, 0)

        def gain(s, _):
            d = d_ref[pl.ds(s, GROUP, stride=share), :]
            for j in range(degrees):
                row = j * share + s
                rows = pl.ds(pl.multiple_of(row * LANES + begin, GROUP), GROUP)
                for k in range(2):
                    sums = jnp.sum((d * h_ref[rows, k * LANES : (k + 1) * LANES]).reshape(-1, 8, LANES), 0)
                    place = pl.ds(pl.multiple_of((k * LANES + row) * 8, 8), 8)
                    acc_ref[place, :] = acc_ref[place, :] + sums
            return 0

        lax.fori_loop(0, share, gain, 0)

    total = jnp.sum(acc_ref[...].reshape(2 * LANES, 8, LANES), 1)
    a_h, a_m = split2(total)
    a_l = (total - a_h.astype(F32) - a_m.astype(F32)).astype(BF16)
    o_ref[...] = mm(sum_ref[...], a_h, NT) + mm(sum_ref[...], a_m, NT) + mm(sum_ref[...], a_l, NT)
    sent = pl.ds(1, n - 1)
    pltpu.make_async_remote_copy(
        src_ref=send_ref.at[sent],
        dst_ref=recv_ref.at[sent],
        send_sem=ssem,
        recv_sem=rsem.at[0],
        device_id=peer(1)[1],
        device_id_type=MESH,
    ).wait_send()


def sums_of(maps, deltas, spins, position, ell_index, n):
    degrees, slots, half = deltas.shape
    share = slots * half // position.shape[0]
    length = position.shape[0]
    dma = pltpu.SemaphoreType.DMA
    return pl.pallas_call(
        kernel,
        out_shape=jax.ShapeDtypeStruct((8, 2 * LANES), F32),
        in_specs=[ANY] * 3 + [SMEM, SMEM] + [VMEM] * 9,
        out_specs=VMEM,
        scratch_shapes=[
            pltpu.VMEM((4, SPLIT, length), BF16),
            pltpu.VMEM((length, 2 * LANES), BF16),
            pltpu.VMEM((length, 2 * LANES), BF16),
            pltpu.VMEM((length, LANES), F32),
            pltpu.VMEM((n, share, LANES), I16),
            pltpu.VMEM((n, share, LANES), I16),
            pltpu.VMEM((1, LANES), F32),
            pltpu.VMEM((n, 1, LANES), F32),
            pltpu.VMEM((degrees, share, length), BF16),
            pltpu.VMEM((2, degrees, length), BF16),
            pltpu.VMEM((length, LANES), F32),
            pltpu.VMEM((SPLIT * 2 * degrees, LANES), F32),
            pltpu.VMEM((n, 2 * LANES), F32),
            pltpu.VMEM((LANES * LANES, 2 * LANES), F32),
            pltpu.VMEM((GROUP * share, LANES), F32),
            pltpu.VMEM((2 * LANES * 8, LANES), F32),
            dma((3,)),
            dma((3,)),
            dma((3,)),
            dma,
            dma((n // GROUP,)),
            dma,
            dma,
        ],
        compiler_params=pltpu.CompilerParams(
            collective_id=0, has_side_effects=True, vmem_limit_bytes=56 * 2**20
        ),
        name="coefficient_sums",
    )(maps, deltas, spins, position, ell_index, *tables())


def on_device(maps, deltas, spin_rows, ell_index, owner_map, prior):
    thetas, phis = lax.axis_size("theta"), lax.axis_size("phi")
    theta, phi = lax.axis_index("theta"), lax.axis_index("phi")
    half = maps.shape[2]
    length = half * phis
    n = thetas * phis
    degrees = deltas.shape[1]
    share = deltas.shape[2] // phis
    position = (owner_map & (SPLIT - 1)) * LANES + owner_map // SPLIT
    sums = sums_of(maps, deltas.transpose(1, 2, 0), spin_rows.transpose(1, 2, 0), position, ell_index, n)

    sums = sums[:4].reshape(4, 2, degrees, share)
    scalar_real, scalar_imag = sums[0, 0] - sums[2, 1], sums[2, 0] + sums[0, 1]
    spin_real, spin_imag = sums[1, 0] - sums[3, 1], sums[3, 0] + sums[1, 1]
    ids = lax.dynamic_slice_in_dim(owner_map, (theta * phis + phi) * share, share)
    slot_freq = jnp.where(ids < length // 2, ids, ids - length)
    ell = ell_index.astype(F32)
    weight = 2.0 * math.pi / length * jnp.sqrt((2.0 * ell + 1.0) / (4.0 * math.pi)) / length
    keep = jnp.where(jnp.abs(slot_freq)[None, :] <= ell_index[:, None], weight[:, None], 0.0)
    coupling = (prior * jnp.sqrt(ell * (ell + 1.0)) / (length // 2))[:, None]
    inner_real = (-spin_imag - coupling * scalar_real) * keep
    inner_imag = (spin_real - coupling * scalar_imag) * keep
    turns = jnp.mod(-slot_freq, 4)
    phase_real = jnp.where(turns == 0, 1.0, jnp.where(turns == 2, -1.0, 0.0)).astype(F32)[None, :]
    phase_imag = jnp.where(turns == 1, 1.0, jnp.where(turns == 3, -1.0, 0.0)).astype(F32)[None, :]
    out_real = phase_real * inner_real - phase_imag * inner_imag
    out_imag = phase_real * inner_imag + phase_imag * inner_real
    return jnp.stack([out_real, out_imag], axis=1)


def solution(mesh):
    placed = (
        P("grp", "theta", "phi"),
        P("phi", None, "theta"),
        P("phi", None, None),
        P(),
        P(),
        P(),
    )
    return jax.shard_map(
        on_device,
        mesh=mesh,
        in_specs=placed,
        out_specs=P("grp", None, ("theta", "phi")),
        check_vma=False,
    )
```

```python
import math

import jax
import jax.numpy as jnp
import numpy as np
from jax import lax
from jax.experimental import pallas as pl
from jax.experimental.pallas import tpu as pltpu
from jax.sharding import PartitionSpec as P

F32, BF16, I16 = jnp.float32, jnp.bfloat16, jnp.int16
MESH = pl.DeviceIdType.MESH
VMEM = pl.BlockSpec(memory_space=pltpu.VMEM)
SMEM = pl.BlockSpec(memory_space=pltpu.SMEM)
ANY = pl.BlockSpec(memory_space=pl.ANY)
NN = (((1,), (0,)), ((), ()))
NT = (((1,), (1,)), ((), ()))
TN = (((0,), (0,)), ((), ()))
LANES = 128
SPLIT = 32
HALF = LANES // 2
GROUP = 32
UNROLL = 2
CODE_TOP = 32700.0


def halves(table):
    high = table.astype(jnp.bfloat16)
    low = (table - high.astype(np.float64)).astype(jnp.bfloat16)
    return jnp.asarray(high), jnp.asarray(low)


def turn(product, modulus):
    angle = 2.0 * np.pi / modulus * np.mod(product, modulus)
    return np.cos(angle), np.sin(angle)


def tables():
    step = np.arange(SPLIT)
    lane = np.arange(LANES)
    cos_a, sin_a = turn(np.outer(step, step), SPLIT)
    spread_h, spread_l = halves(np.kron(np.concatenate([cos_a, sin_a]), np.eye(8)))
    cos_t, sin_t = turn(np.outer(step, lane), SPLIT * LANES)
    row_turn = np.stack([np.repeat(cos_t, 8, 0), np.repeat(sin_t, 8, 0)])
    cos_b, sin_b = turn(np.outer(lane, lane), LANES)
    wide = np.concatenate([cos_b, sin_b], 1)
    wide_h, wide_l = halves(wide)
    fold_h, fold_l = halves(np.concatenate([np.kron(np.eye(2), cos_a), np.kron(np.eye(2), -sin_a)], 1))
    cos_k, sin_k = turn(np.outer(lane, step), SPLIT * LANES)
    slot_turn = np.stack([np.tile(cos_k, (1, 4)), np.concatenate([sin_k, sin_k, -sin_k, -sin_k], 1)])
    gather = np.zeros((8, LANES))
    gather[lane // SPLIT, lane] = 1.0
    return (
        spread_h,
        spread_l,
        jnp.asarray(row_turn, F32),
        wide_h,
        wide_l,
        jnp.asarray(wide, F32),
        jnp.concatenate([fold_h, fold_h, fold_l]),
        jnp.asarray(slot_turn, F32),
        jnp.asarray(gather, BF16),
    )


def split2(value):
    high = value.astype(BF16)
    return high, (value - high.astype(F32)).astype(BF16)


def mm(left, right, dims=NN):
    return lax.dot_general(left, right, dims, preferred_element_type=F32)


def mm3(left_h, left_l, right_h, right_l, dims=NN):
    return mm(left_h, right_h, dims) + mm(left_h, right_l, dims) + mm(left_l, right_h, dims)


def row_spectra(x_ref, sh_ref, sl_ref, tw_ref, wh_ref, wl_ref, yh_ref, yl_ref, rt_ref):
    cos_t, sin_t = tw_ref[0], tw_ref[1]

    def columns(z, i):
        return jnp.concatenate([z[8 * i : 8 * i + 8, LANES * a : LANES * (a + 1)] for a in range(SPLIT)], 0)

    def put(h, field, re_parts, im_parts):
        turned = []
        for re, im in zip(re_parts, im_parts):
            turned.append((re * cos_t + im * sin_t, im * cos_t - re * sin_t))
        for k1 in range(SPLIT):
            cut = slice(8 * k1, 8 * k1 + 8)
            re = jnp.concatenate([turned[0][0][cut], turned[1][0][cut]], 0)
            im = jnp.concatenate([turned[0][1][cut], turned[1][1][cut]], 0)
            re_h, re_l = split2(re)
            im_h, im_l = split2(im)
            top = pl.ds(k1 * LANES + field * SPLIT + 16 * h, 16)
            low = pl.ds(k1 * LANES + HALF + field * SPLIT + 16 * h, 16)
            yh_ref[top, :LANES] = re_h
            yh_ref[top, LANES:] = im_h
            yh_ref[low, :LANES] = im_h
            yh_ref[low, LANES:] = -re_h
            yl_ref[top, :LANES] = re_l
            yl_ref[top, LANES:] = im_l
            yl_ref[low, :LANES] = im_l
            yl_ref[low, LANES:] = -re_l

    row_id = lax.broadcasted_iota(jnp.int32, (16, LANES), 0)
    lane_id = lax.broadcasted_iota(jnp.int32, (16, LANES), 1)
    bound = jnp.zeros((1, LANES), F32)
    for h in range(2):
        rows = pl.ds(16 * h, 16)
        v0, v1, v2, v3 = (x_ref[plane, rows, :].astype(F32) for plane in range(4))
        q_re, q_im = v1 * v2, v1 * v3
        sizes = jnp.sum(jnp.abs(v0), 1, keepdims=True), jnp.sum(jnp.abs(q_re) + jnp.abs(q_im), 1, keepdims=True)
        for field in range(2):
            here = lane_id % HALF == row_id + (field * SPLIT + 16 * h)
            bound = bound + jnp.sum(jnp.where(here, sizes[field], 0.0), 0, keepdims=True)
        flat = jnp.concatenate([columns(v0, 0), columns(v0, 1)], 1).astype(BF16)
        out = mm(sh_ref[...], flat) + mm(sl_ref[...], flat)
        put(h, 0, [out[:256, :LANES], out[:256, LANES:]], [-out[256:, :LANES], -out[256:, LANES:]])
        re_parts, im_parts = [], []
        for i in range(2):
            q_h, q_l = split2(jnp.concatenate([columns(q_re, i), columns(q_im, i)], 1))
            out = mm3(sh_ref[...], sl_ref[...], q_h, q_l)
            re_parts.append(out[:256, :LANES] + out[256:, LANES:])
            im_parts.append(out[:256, LANES:] - out[256:, :LANES])
        put(h, 1, re_parts, im_parts)

    def second(step, _):
        rows = pl.ds(pl.multiple_of(step * 256, 256), 256)
        out = mm3(wh_ref[...], wl_ref[...], yh_ref[rows, :], yl_ref[rows, :], NT)
        rt_ref[pl.ds(pl.multiple_of(step * 256, 256), LANES), :] = out[:, :LANES]
        rt_ref[pl.ds(pl.multiple_of(step * 256 + LANES, LANES), LANES), :] = out[:, LANES:]
        return 0

    lax.fori_loop(0, SPLIT // 2, second, 0)
    return jnp.maximum(bound, 1e-30)


def kernel(
    maps_ref, delta_ref, spin_ref, pos_ref, ell_ref, sh_ref, sl_ref, tw_ref, wh_ref, wl_ref, wide_ref, fold_ref, st_ref, sum_ref,
    o_ref,
    x_ref, yh_ref, yl_ref, rt_ref, send_ref, recv_ref, bound_ref, bounds_ref, tab_ref, w_ref, t_ref, wt_ref,
    mine_ref, mh_ref, ml_ref, h_ref, d_ref, acc_ref, near_sem, far_sem, out_sem, ssem, rsem, bsem, brsem,
):
    theta, phi = lax.axis_index("theta"), lax.axis_index("phi")
    phis = lax.axis_size("phi")
    n, share = recv_ref.shape[0], recv_ref.shape[1]
    me = theta * phis + phi
    other = phis - 1 - phi
    half = maps_ref.shape[2]
    here = pl.ds(pl.multiple_of(phi * half, half), half)

    def peer(i):
        j = lax.rem(me + i, n)
        return j, {"theta": lax.div(j, phis), "phi": lax.rem(j, phis)}

    def cut(whose):
        return pl.ds(pl.multiple_of(whose * share, share), share)

    pieces = (
        (lambda whose: maps_ref.at[:, cut(whose), :], x_ref.at[:, :, here]),
        (lambda whose: delta_ref.at[:, cut(whose), :], tab_ref.at[:, :, here]),
        (lambda whose: spin_ref, w_ref.at[:, :, here]),
    )
    near = [pltpu.make_async_copy(src(phi), dst, near_sem.at[k]) for k, (src, dst) in enumerate(pieces)]
    far = [
        pltpu.make_async_remote_copy(
            src_ref=src(other),
            dst_ref=dst,
            send_sem=out_sem.at[k],
            recv_sem=far_sem.at[k],
            device_id={"phi": other},
            device_id_type=MESH,
        )
        for k, (src, dst) in enumerate(pieces)
    ]
    near[0].start()

    barrier = pltpu.get_barrier_semaphore()

    def greet(i):
        pl.semaphore_signal(barrier, inc=1, device_id=peer(i)[1], device_id_type=MESH)

    def greet_some(step, _):
        for k in range(7):
            greet(1 + step * 7 + k)
        return 0

    lax.fori_loop(0, (n - 1) // 7, greet_some, 0)
    for k in range(1 + (n - 1) // 7 * 7, n):
        greet(k)
    pl.semaphore_wait(barrier, n - 1)
    for copy in far:
        copy.start()
    for copy in near[1:]:
        copy.start()
    near[0].wait()
    far[0].wait()

    bound = row_spectra(x_ref, sh_ref, sl_ref, tw_ref, wh_ref, wl_ref, yh_ref, yl_ref, rt_ref)
    bound_ref[...] = bound
    bounds_ref[0] = bound
    shrink = 1.0 / bound

    def encoded(dest, target, slot):
        for part in range(share // 16):
            base = dest * share + part * 16
            rows = [rt_ref[pl.ds(pos_ref[base + i], 1), :] for i in range(16)]
            x = jnp.concatenate(rows, 0)
            code = jnp.sqrt(jnp.abs(x) * shrink) * CODE_TOP + 0.5
            code = jnp.where(x < 0.0, -code, code).astype(jnp.int32)
            target[slot, 16 * part : 16 * part + 16, :] = code.astype(I16)

    def post(i):
        where = peer(i)[1]
        pltpu.make_async_remote_copy(
            src_ref=bound_ref,
            dst_ref=bounds_ref.at[i],
            send_sem=bsem,
            recv_sem=brsem,
            device_id=where,
            device_id_type=MESH,
        ).start()
        pltpu.make_async_remote_copy(
            src_ref=send_ref.at[i],
            dst_ref=recv_ref.at[i],
            send_sem=ssem,
            recv_sem=rsem.at[i // GROUP],
            device_id=where,
            device_id_type=MESH,
        ).start()

    def fill(i):
        encoded(peer(i)[0], send_ref, i)

    middle = n // 2
    fill(middle)
    fill(1)
    fill(middle + 1)
    post(middle)

    def ship(step, _):
        base = 2 + step * UNROLL
        for k in range(UNROLL):
            i = base + k
            post(i - 1)
            post(middle + i - 1)
            fill(i)
            fill(middle + i)
        return 0

    lax.fori_loop(0, (middle - 2) // UNROLL, ship, 0)
    post(middle - 1)
    post(n - 1)
    encoded(me, recv_ref, 0)

    for copy in near[1:]:
        copy.wait()
    for copy in far[1:]:
        copy.wait()
    degrees, length = tab_ref.shape[0], tab_ref.shape[2]

    def arrange(kh, _):
        lanes = pl.ds(pl.multiple_of(kh * LANES, LANES), LANES)
        for j in range(degrees):
            rows = pl.ds(pl.multiple_of(kh * LANES + j * share, share), share)
            t_ref[rows, :] = tab_ref[j, :, lanes].astype(F32)
        w = jnp.concatenate([w_ref[f, :, lanes].astype(F32) for f in range(2)], 0)
        place = kh * LANES + lax.broadcasted_iota(jnp.int32, w.shape, 1)
        freq = jnp.where(place < length // 2, place, place - length)
        row = lax.broadcasted_iota(jnp.int32, w.shape, 0) % degrees
        ell = jnp.zeros(w.shape, jnp.int32)
        for j in range(degrees):
            ell = jnp.where(row == j, ell_ref[j], ell)
        wt_ref[pl.ds(pl.multiple_of(kh * 8, 8), 8), :] = jnp.where(jnp.abs(freq) <= ell, w, 0.0)
        return 0

    lax.fori_loop(0, SPLIT, arrange, 0)

    def order(i, _):
        mine_ref[pl.ds(i, 1), :] = wide_ref[pl.ds((me - i + n) % n, 1), :]
        return 0

    lax.fori_loop(0, n, order, 0)
    mh_ref[...], ml_ref[...] = split2(mine_ref[...])
    lane_id = lax.broadcasted_iota(jnp.int32, (1, LANES), 1)
    first = lane_id < HALF
    sign = jnp.where(first, 1.0, -1.0).astype(F32)

    def fold(pair, _):
        tops = []
        for i in range(2):
            js = 2 * pair + i
            j = js // share
            t = t_ref[pl.ds(js, SPLIT, stride=LANES), :]
            both = [t * wt_ref[pl.ds(f * degrees + j, SPLIT, stride=8), :] for f in range(2)]
            t_h, t_l = split2(jnp.concatenate(both, 0))
            v = mm(jnp.concatenate([t_h, t_l, t_h], 0), fold_ref[...], TN)
            tops.append(v * st_ref[0] + pltpu.roll(v, HALF, 1) * st_ref[1])
        lows = [pltpu.roll(u, HALF, 1) * sign for u in tops]
        r_h, r_l = split2(jnp.concatenate([jnp.concatenate(tops, 1), jnp.concatenate(lows, 1)], 0))
        out = mm3(mh_ref[...], ml_ref[...], r_h, r_l)
        for i in range(2):
            g = out[:, i * LANES : (i + 1) * LANES]
            back = pltpu.roll(g, HALF, 1)
            rows = pl.ds(pl.multiple_of((2 * pair + i) * LANES, LANES), LANES)
            h_ref[rows, :LANES] = jnp.where(first, g, back)
            h_ref[rows, LANES:] = jnp.where(first, back, g)
        return 0

    def fold_two(step, _):
        fold(2 * step, 0)
        fold(2 * step + 1, 0)
        return 0

    lax.fori_loop(0, LANES // 4, fold_two, 0)
    acc_ref[...] = jnp.zeros_like(acc_ref)

    rest = pl.ds(1, n - 1)
    bounds = pltpu.make_async_remote_copy(
        src_ref=bounds_ref.at[rest],
        dst_ref=bounds_ref.at[rest],
        send_sem=bsem,
        recv_sem=brsem,
        device_id=peer(1)[1],
        device_id_type=MESH,
    )
    bounds.wait_send()
    bounds.wait_recv()
    groups = n // GROUP
    for group in [k // 2 + k % 2 * (groups // 2) for k in range(groups)]:
        begin = group * GROUP
        part = pl.ds(max(begin, 1), GROUP - (begin == 0))
        pltpu.make_async_remote_copy(
            src_ref=send_ref.at[part],
            dst_ref=recv_ref.at[part],
            send_sem=ssem,
            recv_sem=rsem.at[group],
            device_id=peer(1)[1],
            device_id_type=MESH,
        ).wait_recv()

        def widen(k, _):
            slot = begin + k
            code = recv_ref[slot].astype(jnp.int32).astype(F32)
            grow = bounds_ref[slot] * (1.0 / CODE_TOP**2)
            d_ref[pl.ds(pl.multiple_of(k * share, share), share), :] = code * jnp.abs(code) * grow
            return 0

        lax.fori_loop(0, GROUP, widen, 0)

        def gain(s, _):
            d = d_ref[pl.ds(s, GROUP, stride=share), :]
            for j in range(degrees):
                row = j * share + s
                rows = pl.ds(pl.multiple_of(row * LANES + begin, GROUP), GROUP)
                for k in range(2):
                    sums = jnp.sum((d * h_ref[rows, k * LANES : (k + 1) * LANES]).reshape(-1, 8, LANES), 0)
                    place = pl.ds(pl.multiple_of((k * LANES + row) * 8, 8), 8)
                    acc_ref[place, :] = acc_ref[place, :] + sums
            return 0

        lax.fori_loop(0, share, gain, 0)

    total = jnp.sum(acc_ref[...].reshape(2 * LANES, 8, LANES), 1)
    a_h, a_m = split2(total)
    a_l = (total - a_h.astype(F32) - a_m.astype(F32)).astype(BF16)
    o_ref[...] = mm(sum_ref[...], a_h, NT) + mm(sum_ref[...], a_m, NT) + mm(sum_ref[...], a_l, NT)
    sent = pl.ds(1, n - 1)
    pltpu.make_async_remote_copy(
        src_ref=send_ref.at[sent],
        dst_ref=recv_ref.at[sent],
        send_sem=ssem,
        recv_sem=rsem.at[0],
        device_id=peer(1)[1],
        device_id_type=MESH,
    ).wait_send()


def sums_of(maps, deltas, spins, position, ell_index, n):
    degrees, slots, half = deltas.shape
    share = slots * half // position.shape[0]
    length = position.shape[0]
    dma = pltpu.SemaphoreType.DMA
    return pl.pallas_call(
        kernel,
        out_shape=jax.ShapeDtypeStruct((8, 2 * LANES), F32),
        in_specs=[ANY] * 3 + [SMEM, SMEM] + [VMEM] * 9,
        out_specs=VMEM,
        scratch_shapes=[
            pltpu.VMEM((4, SPLIT, length), BF16),
            pltpu.VMEM((length, 2 * LANES), BF16),
            pltpu.VMEM((length, 2 * LANES), BF16),
            pltpu.VMEM((length, LANES), F32),
            pltpu.VMEM((n, share, LANES), I16),
            pltpu.VMEM((n, share, LANES), I16),
            pltpu.VMEM((1, LANES), F32),
            pltpu.VMEM((n, 1, LANES), F32),
            pltpu.VMEM((degrees, share, length), BF16),
            pltpu.VMEM((2, degrees, length), BF16),
            pltpu.VMEM((length, LANES), F32),
            pltpu.VMEM((SPLIT * 2 * degrees, LANES), F32),
            pltpu.VMEM((n, 2 * LANES), F32),
            pltpu.VMEM((n, 2 * LANES), BF16),
            pltpu.VMEM((n, 2 * LANES), BF16),
            pltpu.VMEM((LANES * LANES, 2 * LANES), F32),
            pltpu.VMEM((GROUP * share, LANES), F32),
            pltpu.VMEM((2 * LANES * 8, LANES), F32),
            dma((3,)),
            dma((3,)),
            dma((3,)),
            dma,
            dma((n // GROUP,)),
            dma,
            dma,
        ],
        compiler_params=pltpu.CompilerParams(
            collective_id=0, has_side_effects=True, vmem_limit_bytes=56 * 2**20
        ),
        name="coefficient_sums",
    )(maps, deltas, spins, position, ell_index, *tables())


def on_device(maps, deltas, spin_rows, ell_index, owner_map, prior):
    thetas, phis = lax.axis_size("theta"), lax.axis_size("phi")
    theta, phi = lax.axis_index("theta"), lax.axis_index("phi")
    half = maps.shape[2]
    length = half * phis
    n = thetas * phis
    degrees = deltas.shape[1]
    share = deltas.shape[2] // phis
    position = (owner_map & (SPLIT - 1)) * LANES + owner_map // SPLIT
    sums = sums_of(maps, deltas.transpose(1, 2, 0), spin_rows.transpose(1, 2, 0), position, ell_index, n)

    sums = sums[:4].reshape(4, 2, degrees, share)
    scalar_real, scalar_imag = sums[0, 0] - sums[2, 1], sums[2, 0] + sums[0, 1]
    spin_real, spin_imag = sums[1, 0] - sums[3, 1], sums[3, 0] + sums[1, 1]
    ids = lax.dynamic_slice_in_dim(owner_map, (theta * phis + phi) * share, share)
    slot_freq = jnp.where(ids < length // 2, ids, ids - length)
    ell = ell_index.astype(F32)
    weight = 2.0 * math.pi / length * jnp.sqrt((2.0 * ell + 1.0) / (4.0 * math.pi)) / length
    keep = jnp.where(jnp.abs(slot_freq)[None, :] <= ell_index[:, None], weight[:, None], 0.0)
    coupling = (prior * jnp.sqrt(ell * (ell + 1.0)) / (length // 2))[:, None]
    inner_real = (-spin_imag - coupling * scalar_real) * keep
    inner_imag = (spin_real - coupling * scalar_imag) * keep
    turns = jnp.mod(-slot_freq, 4)
    phase_real = jnp.where(turns == 0, 1.0, jnp.where(turns == 2, -1.0, 0.0)).astype(F32)[None, :]
    phase_imag = jnp.where(turns == 1, 1.0, jnp.where(turns == 3, -1.0, 0.0)).astype(F32)[None, :]
    out_real = phase_real * inner_real - phase_imag * inner_imag
    out_imag = phase_real * inner_imag + phase_imag * inner_real
    return jnp.stack([out_real, out_imag], axis=1)


def solution(mesh):
    placed = (
        P("grp", "theta", "phi"),
        P("phi", None, "theta"),
        P("phi", None, None),
        P(),
        P(),
        P(),
    )
    return jax.shard_map(
        on_device,
        mesh=mesh,
        in_specs=placed,
        out_specs=P("grp", None, ("theta", "phi")),
        check_vma=False,
    )
```
